256 devices in a mesh: seq: 64 (over x_hi, z, y), mp: 4 (over x_lo, core).
Axes of the slice: x: 4 (x_hi: 2, x_lo: 2; x = x_hi * 2 + x_lo), y: 4, z: 8, core: 2. Of those that a mesh axis runs over, the one named last changes fastest.
Arguments:
- gate_in: bfloat16 [65536, 1024], P('seq', 'mp'), may hold values from -5 to 5
- value_in: bfloat16 [65536, 1024], P('seq', 'mp'), may hold values from -5 to 5
- out_gate: bfloat16 [65536, 1024], P('seq', 'mp'), may hold values from -10 to 10
- filter_taps: bfloat16 [4096, 1024], P('seq', 'mp'), may hold values from -0.09375 to 0.09375
- skip_gain: float32 [1024], P('mp'), may hold values from -4 to 4
Outputs:
- output: bfloat16 [65536, 1024], P('seq', 'mp')
The draws below stay inside these ranges and needn't reach their ends.
All inputs are finite; a program needn't handle non-finite values.
Results may differ from the reference program's by a relative error of at most 0.009.
Values may be sent and summed in bfloat16 or wider, within the bound.
No kernel may reach another device: no remote copies, remote signals or barrier semaphores. Data moves between devices by JAX's collectives and lax.ppermute only.
A program may use at most 64 MiB of HBM per device.

```python
import math
import jax
import jax.numpy as jnp
from jax import lax

C = 1024
K = 4096
TOKENS = 65536


def draw_out_gate(key, part):
    first_key, second_key = jax.random.split(jax.random.fold_in(key, 11), 2)
    position = jnp.arange(C, dtype=jnp.float32) / (C - 1)
    ramp = 0.55 * jnp.power(3.0, position)
    channel_scale = jnp.exp(jax.random.uniform(second_key, (C,), jnp.float32, math.log(0.7), math.log(1.4)))
    base = jnp.clip(jax.random.normal(first_key, (TOKENS, C), jnp.float32), -4.0, 4.0)
    return (base * ramp[None, :] * channel_scale[None, :]).astype(jnp.bfloat16)


def block_scale(key, dims, pieces, smallest, largest):
    def one(dim, parts):
        draws = jax.random.uniform(jax.random.fold_in(jax.random.fold_in(key, 6), dim), (parts,), jnp.float32, smallest / len(pieces), largest / len(pieces))
        return jnp.repeat(jnp.exp(draws), dims[dim] // parts).reshape((-1,) + (1,) * (len(dims) - dim - 1))

    loudness = one(*pieces[0])
    for cut in pieces[1:]:
        loudness = loudness * one(*cut)
    return loudness


def gaussian(stream_key, extent, scale, bound, cuts=(), held_as=jnp.bfloat16):
    loudness = block_scale(stream_key, extent, cuts, -0.22, 0.18) if cuts else 1.0
    entries = jax.random.normal(stream_key, extent, jnp.float32) * scale * loudness
    return jnp.minimum(jnp.maximum(entries, -bound), bound).astype(held_as)


def setup_inputs(seed: int = 0) -> dict:
    keys = jax.random.split(jax.random.key(seed), 6)
    return {
        "gate_in": gaussian(keys[0], (TOKENS, C), 1.0, 5.0, ((0, 64), (1, 4))),
        "value_in": gaussian(keys[1], (TOKENS, C), 1.0, 5.0, ((0, 64), (1, 4))),
        "out_gate": draw_out_gate(jax.random.fold_in(keys[5], 71), 0),
        "filter_taps": gaussian(keys[3], (K, C), K ** -0.5, 0.09375, ((0, 64), (1, 4))),
        "skip_gain": gaussian(keys[4], (C,), 1.0, 4.0, ((0, 4),), jnp.float32),
    }


def convolve_group(signal_kernel):
    signal, kernel = signal_kernel
    length = signal.shape[1]
    size = 1 << (length + kernel.shape[1] - 1).bit_length()
    product = jnp.fft.rfft(signal, size) * jnp.fft.rfft(kernel, size)
    return jnp.fft.irfft(product, size)[:, :length]

def reference(gate_in, value_in, out_gate, filter_taps, skip_gain):
    gated = (gate_in.astype(jnp.float32) * value_in.astype(jnp.float32)).astype(jnp.bfloat16)
    group = 32
    signal = gated.astype(jnp.float32).T.reshape(C // group, group, TOKENS)
    kernel = filter_taps.astype(jnp.float32).T.reshape(C // group, group, K)
    convolved = lax.map(convolve_group, (signal, kernel)).reshape(C, TOKENS).T
    mixed = out_gate.astype(jnp.float32) * (convolved + skip_gain[None, :] * gated.astype(jnp.float32))
    power = lax.optimization_barrier(jnp.mean(mixed * mixed, axis=1, keepdims=True))
    return (mixed / jnp.sqrt(power + 1e-05)).astype(jnp.bfloat16)
```

```python
import functools
import jax
import jax.numpy as jnp
from jax import lax
from jax.experimental import pallas as pl
from jax.experimental.pallas import tpu as pltpu
from jax.sharding import PartitionSpec as P

CH = 1024
TAPS = 4096
BLOCK = 256
LAGS = TAPS // BLOCK
NT = (((1,), (1,)), ((), ()))
F32 = jnp.float32
BF16 = jnp.bfloat16


def identity(n):
    row = lax.broadcasted_iota(jnp.int32, (n, n), 0)
    col = lax.broadcasted_iota(jnp.int32, (n, n), 1)
    return jnp.where(row == col, 1.0, 0.0).astype(BF16)


def flipped(eye, block):
    return lax.dot_general(eye, block, NT, preferred_element_type=F32)


def gate_kernel(gate_ref, value_ref, taps_ref, out_ref, taps_out_ref, rows_ref):
    tokens, channels = gate_ref.shape
    peers = out_ref.shape[0]
    per_peer = channels // peers
    eye = identity(channels)
    for b in range(tokens // 128):
        part = pl.ds(b * 128, 128)
        gated = (gate_ref[part, :].astype(F32) * value_ref[part, :].astype(F32)).astype(BF16)
        rows_ref[b, :channels, :] = flipped(eye, gated)
    count = tokens // 128
    flat = rows_ref.reshape(count * rows_ref.shape[1], 128)
    pitch = rows_ref.shape[1]
    for j in range(peers):
        got = [flat[pl.ds(q * peers + j, count, stride=pitch), :] for q in range(per_peer)]
        out_ref[j] = jnp.concatenate(got, axis=0).astype(BF16)
    taps_out_ref[...] = flipped(eye, taps_ref[...]).astype(BF16)


def conv_kernel(where_ref, skip_ref, x_ref, taps_ref, out_ref, flat_ref, even_ref, odd_ref, wide_ref, out_rows):
    per_peer = taps_ref.shape[0]
    sources = 64
    segs = 8
    per_seg = sources // segs
    positions = per_seg * 4
    rows = positions * segs
    chunk = per_peer * 8
    pitch = per_seg * chunk + 8
    for g in range(segs):
        flat_ref[pl.ds(g * pitch, per_seg * chunk), :] = x_ref[pl.ds(g * per_seg * chunk, per_seg * chunk), :].astype(F32)
    lane = lax.broadcasted_iota(jnp.int32, (16, 128), 1)
    sub = lax.broadcasted_iota(jnp.int32, (16, 128), 0)
    first = lax.broadcasted_iota(jnp.int32, (8, 128), 0) == 0

    wide_ref[:, :128] = jnp.zeros((128, 128), BF16)
    wide_ref[:, 34 * 128:] = jnp.zeros((128, 128), BF16)

    def channel(q, _):
        before = [jnp.zeros((16, 128), BF16)] * 8
        for j in range(33):
            if j < 32:
                line = jnp.broadcast_to(taps_ref[q, pl.ds(j, 1), :], (16, 128))
                base = pltpu.roll(line, 0, 1, stride=1, stride_axis=0)
                now = [pltpu.roll(base, 16 * i, 1).astype(BF16) if i else base.astype(BF16) for i in range(8)]
            else:
                now = [jnp.zeros((16, 128), BF16)] * 8
            for i in range(8):
                wide_ref[pl.ds(16 * i, 16), pl.ds(128 * (j + 1), 128)] = jnp.where(
                    lane >= sub + 16 * i, now[i], before[i]
                )
            before = now
        tiles = []
        for p in range(positions):
            halves = []
            for h in range(2):
                b = (p % 4) * 2 + h
                start = (p // 4) * chunk + q * 8 + b
                halves.append(flat_ref[pl.ds(start, 8, stride=pitch), :])
            tiles.append(jnp.concatenate(halves, axis=1))
        first2 = jnp.concatenate([first, first], axis=1)
        line = [jnp.where(first2, 0.0, pltpu.roll(tiles[p + positions - LAGS], 1, 0)) for p in range(LAGS)] + tiles
        for a in range(len(line) // 2):
            even_ref[pl.ds(16 * a, 16), :] = jnp.concatenate([line[2 * a], line[2 * a + 1]], axis=0).astype(BF16)
        for a in range(len(line) // 2 - 1):
            odd_ref[pl.ds(16 * a, 16), :] = jnp.concatenate([line[2 * a + 1], line[2 * a + 2]], axis=0).astype(BF16)
        acc = None
        for s in range(LAGS + 1):
            start = LAGS - s
            if start % 2 == 0:
                lhs = even_ref[pl.ds(start * 8, rows), :]
            else:
                lhs = odd_ref[pl.ds((start - 1) * 8, rows), :]
            u = s * BLOCK
            rhs = jnp.concatenate([wide_ref[:, u + 128:u + 384], wide_ref[:, u:u + 256]], axis=0)
            term = jnp.dot(lhs, rhs, preferred_element_type=F32)
            acc = term if acc is None else acc + term
        skip = skip_ref[q * sources + where_ref[0]]
        for p in range(positions):
            full = acc[8 * p:8 * p + 8] + skip * tiles[p]
            for h in range(2):
                out_rows[pl.ds((p * 2 + h) * 8, 8), :] = full[:, h * 128:(h + 1) * 128]
        for g in range(segs):
            for jj in range(per_seg):
                got = out_rows[pl.ds(jj * 64 + g, 8, stride=8), :]
                out_ref[g * per_seg + jj, pl.ds(pl.multiple_of(q * 8, 8), 8), :] = got.astype(BF16)
        return 0

    lax.fori_loop(0, per_peer, channel, 0)


def mix_kernel(conv_ref, og_ref, mixed_ref, square_ref, rows_ref):
    tokens, channels = og_ref.shape
    peers = conv_ref.shape[0]
    per_peer = channels // peers
    count = tokens // 128
    chunk = per_peer * count
    rows_ref[...] = conv_ref[...].reshape(peers * chunk, 128).astype(F32)
    eye = identity(channels)
    for b in range(count):
        gate = flipped(eye, og_ref[pl.ds(b * 128, 128), :])
        total = jnp.zeros((8, 128), F32)
        for q in range(per_peer):
            got = rows_ref[pl.ds(q * count + b, peers, stride=chunk), :]
            mixed = gate[q * peers:(q + 1) * peers] * got
            mixed_ref[b, pl.ds(q * peers, peers), :] = mixed
            total = total + jnp.sum((mixed * mixed).reshape(peers // 8, 8, 128), axis=0)
        square_ref[pl.ds(b, 1), :] = jnp.sum(total, axis=0, keepdims=True)


def norm_kernel(mixed_ref, square_ref, out_ref):
    count, channels, _ = mixed_ref.shape
    power = (square_ref[0] + square_ref[1] + square_ref[2] + square_ref[3]) * (1.0 / CH)
    scale = 1.0 / jnp.sqrt(power + 1e-05)
    eye = identity(128)
    for b in range(count):
        scaled = (mixed_ref[b] * scale[b:b + 1, :]).astype(BF16)
        out_ref[pl.ds(b * 128, 128), :] = flipped(eye, scaled).astype(BF16)


def shape(dims, dtype):
    return jax.ShapeDtypeStruct(dims, dtype)


VMEM = pl.BlockSpec(memory_space=pltpu.VMEM)
SMEM = pl.BlockSpec(memory_space=pltpu.SMEM)


def local(gate_in, value_in, out_gate, filter_taps, skip_gain):
    tokens, channels = gate_in.shape
    peers = lax.axis_size("seq")
    per_peer = channels // peers
    count = tokens // 128
    taps_here = filter_taps.shape[0]
    message, taps = pl.pallas_call(
        gate_kernel,
        out_shape=(shape((peers, per_peer * count, 128), BF16), shape((channels, taps_here), BF16)),
        in_specs=[VMEM] * 3,
        out_specs=(VMEM, VMEM),
        scratch_shapes=[pltpu.VMEM((count, channels + 8, 128), F32)],
        name="gate",
    )(gate_in, value_in, filter_taps)
    tap_rows = taps.reshape(per_peer, peers, taps_here).transpose(1, 0, 2).reshape(peers, 1, 2, 128)
    message = jnp.concatenate([message.reshape(peers, 16, 2, 128), tap_rows], axis=1)
    message = lax.all_to_all(message, "seq", split_axis=0, concat_axis=0, tiled=True)
    signal = message[:, :16].reshape(peers * per_peer * count, 128)
    taps = message[:, 16].reshape(peers, per_peer, taps_here).transpose(1, 0, 2).reshape(per_peer, 32, 128).astype(F32)
    where = lax.axis_index("seq").reshape(1).astype(jnp.int32)
    convolved = pl.pallas_call(
        conv_kernel,
        out_shape=shape((peers, per_peer * count, 128), BF16),
        in_specs=[SMEM, SMEM, VMEM, VMEM],
        out_specs=VMEM,
        scratch_shapes=[
            pltpu.VMEM((8 * (8 * per_peer * count + 8), 128), F32),
            pltpu.VMEM((384, 256), BF16),
            pltpu.VMEM((384, 256), BF16),
            pltpu.VMEM((128, 35 * 128), BF16),
            pltpu.VMEM((512, 128), F32),
        ],
        name="conv",
    )(where, skip_gain, signal, taps)
    convolved = lax.all_to_all(convolved, "seq", split_axis=0, concat_axis=0, tiled=True)
    mixed, squares = pl.pallas_call(
        mix_kernel,
        out_shape=(shape((count, channels, 128), F32), shape((count, 128), F32)),
        in_specs=[VMEM] * 2,
        out_specs=(VMEM, VMEM),
        scratch_shapes=[pltpu.VMEM((peers * per_peer * count, 128), F32)],
        name="mix",
    )(convolved, out_gate)
    squares = lax.all_gather(squares, "mp")
    return pl.pallas_call(
        norm_kernel,
        out_shape=shape((tokens, channels), BF16),
        in_specs=[VMEM] * 2,
        out_specs=VMEM,
        name="norm",
    )(mixed, squares)


def solution(mesh):
    return jax.shard_map(
        local,
        mesh=mesh,
        in_specs=(P("seq", "mp"), P("seq", "mp"), P("seq", "mp"), P("seq", "mp"), P("mp")),
        out_specs=P("seq", "mp"),
        check_vma=False,
    )
```

```python
import jax
import jax.numpy as jnp
from jax import lax
from jax.experimental import pallas as pl
from jax.experimental.pallas import tpu as pltpu
from jax.sharding import PartitionSpec as P

CH = 1024
TAPS = 4096
BLOCK = 256
LAGS = TAPS // BLOCK
SEGS = 8
NT = (((1,), (1,)), ((), ()))
F32 = jnp.float32
BF16 = jnp.bfloat16
MIB = 1024 * 1024


def identity(n):
    row = lax.broadcasted_iota(jnp.int32, (n, n), 0)
    col = lax.broadcasted_iota(jnp.int32, (n, n), 1)
    return jnp.where(row == col, 1.0, 0.0).astype(BF16)


def flipped(eye, block):
    return lax.dot_general(eye, block, NT, preferred_element_type=F32)


def gate_kernel(gated_ref, og_ref, taps_ref, skip_ref, out_ref, og_out_ref, skip_out_ref, rows_ref, og_rows_ref):
    skip_out_ref[...] = skip_ref[...]
    tokens, channels = gated_ref.shape
    count = tokens // 128
    pitch = og_rows_ref.shape[0] // count
    chunk = 34
    peers = out_ref.shape[0] // chunk
    per_peer = channels // peers
    eye = identity(channels)
    turned = flipped(eye, taps_ref[...])
    wide = (2 * count + 8) * pitch
    for r in range(2):
        rows_ref[pl.ds(wide + r * (peers + 8), peers), :] = jnp.concatenate(
            [turned[2 * r * peers:(2 * r + 1) * peers], turned[(2 * r + 1) * peers:(2 * r + 2) * peers]], axis=1
        )
    front = 8 * pitch
    for b in range(0, count, 2):
        turned = flipped(eye, gated_ref[pl.ds(b * 128, 256), :])
        for n in range(2):
            rows_ref[pl.ds(front + (b + n) * pitch, channels), :] = turned[:, n * 128:(n + 1) * 128]
        turned = flipped(eye, og_ref[pl.ds(b * 128, 256), :])
        for n in range(2):
            og_rows_ref[pl.ds((b + n) * pitch, channels), :] = turned[:, n * 128:(n + 1) * 128]
    sub = lax.broadcasted_iota(jnp.int32, (8, 128), 0)

    def tile(first):
        runs = []
        row = first
        while row < first + 8:
            j, r = divmod(row, chunk)
            at = row - first
            if r < 32:
                q, b = divmod(r, count)
                base = front + q * peers + j + (b - at) * pitch
                runs.append((at, rows_ref[pl.ds(base, 8, stride=pitch), :]))
                row += count - b
            else:
                base = wide + j + (r - 32 - at) * (peers + 8)
                runs.append((at, rows_ref[pl.ds(base, 8, stride=peers + 8), :]))
                row += 34 - r
        value = runs[0][1]
        for at, more in runs[1:]:
            value = jnp.where(sub >= at, more, value)
        return value

    for n in range(peers * chunk // 16):
        out_ref[pl.ds(n * 16, 16), :] = jnp.concatenate([tile(n * 16), tile(n * 16 + 8)], axis=0).astype(BF16)
    for j in range(peers):
        got = [og_rows_ref[pl.ds(q * peers + j, count, stride=pitch), :] for q in range(per_peer)]
        og_out_ref[pl.ds(j * 32, 32), :] = jnp.concatenate(got, axis=0).astype(BF16)


def conv_kernel(skip_ref, x_ref, out_ref, flat_ref, taps_ref, even_ref, odd_ref, wide_ref, out_rows):
    chunk = 34
    sources = x_ref.shape[0] // chunk
    per_peer = 4
    per_seg = sources // SEGS
    positions = per_seg * 4
    rows = positions * SEGS
    pitch = flat_ref.shape[0] // SEGS
    for g in range(SEGS):
        flat_ref[pl.ds(g * pitch, per_seg * chunk), :] = x_ref[pl.ds(g * per_seg * chunk, per_seg * chunk), :].astype(F32)
    low = lax.broadcasted_iota(jnp.int32, (4, 128), 1) < 64
    for r in range(2):
        for g in range(SEGS):
            even = flat_ref[pl.ds(g * pitch + 32 + r, 4, stride=2 * chunk), :]
            odd = flat_ref[pl.ds(g * pitch + chunk + 32 + r, 4, stride=2 * chunk), :]
            taps_ref[2 * r, pl.ds(4 * g, 4), :] = jnp.where(low, even, pltpu.roll(odd, 64, 1))
            taps_ref[2 * r + 1, pl.ds(4 * g, 4), :] = jnp.where(low, pltpu.roll(even, 64, 1), odd)
    lane = lax.broadcasted_iota(jnp.int32, (16, 128), 1)
    sub = lax.broadcasted_iota(jnp.int32, (16, 128), 0)
    first = lax.broadcasted_iota(jnp.int32, (8, 256), 0) == 0
    for q in range(per_peer):
        wide_ref[q, :, :128] = jnp.zeros((128, 128), BF16)
        wide_ref[q, :, 34 * 128:] = jnp.zeros((128, 128), BF16)

    for q in range(per_peer):
        before = [jnp.zeros((16, 128), BF16)] * 8
        for j in range(33):
            if j < 32:
                line = jnp.broadcast_to(taps_ref[q, pl.ds(j, 1), :], (16, 128))
                base = pltpu.roll(line, 0, 1, stride=1, stride_axis=0)
                now = [pltpu.roll(base, 16 * i, 1).astype(BF16) if i else base.astype(BF16) for i in range(8)]
            else:
                now = [jnp.zeros((16, 128), BF16)] * 8
            for i in range(8):
                wide_ref[q, pl.ds(16 * i, 16), pl.ds(128 * (j + 1), 128)] = jnp.where(
                    lane >= sub + 16 * i, now[i], before[i]
                )
            before = now
        tiles = []
        for p in range(positions):
            halves = []
            for h in range(2):
                start = (p // 4) * chunk + q * 8 + (p % 4) * 2 + h
                halves.append(flat_ref[pl.ds(start, 8, stride=pitch), :])
            tiles.append(jnp.concatenate(halves, axis=1))
        line = [jnp.where(first, 0.0, pltpu.roll(tiles[p + positions - LAGS], 1, 0)) for p in range(LAGS)] + tiles
        for a in range(len(line) // 2):
            even_ref[q, pl.ds(16 * a, 16), :] = jnp.concatenate([line[2 * a], line[2 * a + 1]], axis=0).astype(BF16)
        for a in range(len(line) // 2 - 1):
            odd_ref[q, pl.ds(16 * a, 16), :] = jnp.concatenate([line[2 * a + 1], line[2 * a + 2]], axis=0).astype(BF16)
        acc = None
        for s in range(LAGS + 1):
            start = LAGS - s
            if start % 2 == 0:
                lhs = even_ref[q, pl.ds(start * 8, rows), :]
            else:
                lhs = odd_ref[q, pl.ds((start - 1) * 8, rows), :]
            u = s * BLOCK
            rhs = jnp.concatenate([wide_ref[q, :, u + 128:u + 384], wide_ref[q, :, u:u + 256]], axis=0)
            term = jnp.dot(lhs, rhs, preferred_element_type=F32)
            acc = term if acc is None else acc + term
        mine = lax.broadcasted_iota(jnp.int32, (2, 128), 0) * 128 + lax.broadcasted_iota(jnp.int32, (2, 128), 1)
        mine = jnp.where(mine == q * sources + lax.axis_index("seq"), skip_ref[...], 0.0)
        skip = jnp.sum(jnp.sum(mine, axis=1, keepdims=True), axis=0, keepdims=True)
        for p in range(positions):
            for h in range(2):
                start = (p // 4) * chunk + q * 8 + (p % 4) * 2 + h
                own = flat_ref[pl.ds(start, 8, stride=pitch), :]
                out_rows[q, pl.ds((p * 2 + h) * 8, 8), :] = acc[8 * p:8 * p + 8, h * 128:(h + 1) * 128] + skip * own
    for j in range(sources):
        g, jj = divmod(j, per_seg)
        got = [out_rows[q, pl.ds(jj * 64 + g, 8, stride=8), :] for q in range(per_peer)]
        out_ref[pl.ds(j * 32, 32), :] = jnp.concatenate(got, axis=0).astype(BF16)


def square_kernel(conv_ref, og_ref, square_ref):
    def step(n, total):
        part = pl.ds(pl.multiple_of(n * 128, 128), 128)
        mixed = conv_ref[part, :].astype(F32) * og_ref[part, :].astype(F32)
        return total + (mixed * mixed).reshape(8, 16, 128)

    total = lax.fori_loop(0, conv_ref.shape[0] // 128, step, jnp.zeros((8, 16, 128), F32), unroll=True)
    total = jnp.sum(total, axis=0)
    square_ref[...] = total[:8] + total[8:]


def norm_kernel(conv_ref, og_ref, square_ref, out_hbm, rows_ref, out_ref, sems):
    rows = conv_ref.shape[0]
    tokens, channels = out_ref.shape
    count = tokens // 128
    peers = rows // 32
    per_peer = channels // peers
    power = (square_ref[0] + square_ref[1] + square_ref[2] + square_ref[3]) * (1.0 / CH)
    scale = 1.0 / jnp.sqrt(power + 1e-05)
    scale = jnp.concatenate([scale, scale], axis=0)
    for n in range(rows // 16):
        part = pl.ds(n * 16, 16)
        rows_ref[part, :] = conv_ref[part, :].astype(F32) * og_ref[part, :].astype(F32) * scale
    eye = identity(128)
    copies = []
    for b in range(count):
        got = [rows_ref[pl.ds(q * count + b, peers, stride=32), :] for q in range(per_peer)]
        part = pl.ds(b * 128, 128)
        out_ref[part, :] = flipped(eye, jnp.concatenate(got, axis=0).astype(BF16)).astype(BF16)
        copies.append(pltpu.make_async_copy(out_ref.at[part], out_hbm.at[part], sems.at[b]))
        copies[-1].start()
    for copy in copies:
        copy.wait()


def shape(dims, dtype):
    return jax.ShapeDtypeStruct(dims, dtype)


VMEM = pl.BlockSpec(memory_space=pltpu.VMEM)
SMEM = pl.BlockSpec(memory_space=pltpu.SMEM)
HBM = pl.BlockSpec(memory_space=pltpu.HBM)


def params(mib):
    return pltpu.CompilerParams(vmem_limit_bytes=mib * MIB)


def local(gate_in, value_in, out_gate, filter_taps, skip_gain):
    tokens, channels = gate_in.shape
    peers = lax.axis_size("seq")
    per_peer = channels // peers
    count = tokens // 128
    rows = peers * per_peer * count
    gated = (gate_in.astype(F32) * value_in.astype(F32)).astype(BF16)
    message, turned, skip = pl.pallas_call(
        gate_kernel,
        out_shape=(shape((peers * 34, 128), BF16), shape((rows, 128), BF16), shape((channels // 128, 128), F32)),
        in_specs=[VMEM] * 4,
        out_specs=(VMEM,) * 3,
        scratch_shapes=[
            pltpu.VMEM(((2 * count + 8) * (channels + 8) + 16 * (peers + 8), 128), F32),
            pltpu.VMEM((count * (channels + 8), 128), F32),
        ],
        compiler_params=params(12),
        name="gate",
    )(gated, out_gate, filter_taps, skip_gain.reshape(channels // 128, 128))
    message = lax.all_to_all(message.reshape(peers, 17, 2, 128), "seq", split_axis=0, concat_axis=0, tiled=True)
    convolved = pl.pallas_call(
        conv_kernel,
        out_shape=shape((rows, 128), BF16),
        in_specs=[VMEM, VMEM],
        out_specs=VMEM,
        scratch_shapes=[
            pltpu.VMEM((SEGS * 280, 128), F32),
            pltpu.VMEM((4, 32, 128), F32),
            pltpu.VMEM((4, 384, 256), BF16),
            pltpu.VMEM((4, 384, 256), BF16),
            pltpu.VMEM((4, 128, 35 * 128), BF16),
            pltpu.VMEM((4, 512, 128), F32),
        ],
        compiler_params=params(24),
        name="conv",
    )(skip, message.reshape(peers * 34, 128))
    convolved = lax.all_to_all(
        convolved.reshape(peers, 32, 128), "seq", split_axis=0, concat_axis=0, tiled=True
    ).reshape(rows, 128)
    squares = pl.pallas_call(
        square_kernel,
        out_shape=shape((count, 128), F32),
        in_specs=[VMEM] * 2,
        out_specs=VMEM,
        compiler_params=params(8),
        name="square",
    )(convolved, turned)
    squares = lax.all_gather(squares, "mp")
    return pl.pallas_call(
        norm_kernel,
        out_shape=shape((tokens, channels), BF16),
        in_specs=[VMEM] * 3,
        out_specs=HBM,
        scratch_shapes=[
            pltpu.VMEM((rows, 128), F32),
            pltpu.VMEM((tokens, channels), BF16),
            pltpu.SemaphoreType.DMA((count,)),
        ],
        compiler_params=params(12),
        name="norm",
    )(convolved, turned, squares)


def solution(mesh):
    return jax.shard_map(
        local,
        mesh=mesh,
        in_specs=(P("seq", "mp"), P("seq", "mp"), P("seq", "mp"), P("seq", "mp"), P("mp")),
        out_specs=P("seq", "mp"),
        check_vma=False,
    )
```

```python
import jax
import jax.numpy as jnp
from jax import lax
from jax.experimental import pallas as pl
from jax.experimental.pallas import tpu as pltpu
from jax.sharding import PartitionSpec as P

CH = 1024
TAPS = 4096
BLOCK = 256
LAGS = TAPS // BLOCK
SEGS = 8
ROLLED = 6
NT = (((1,), (1,)), ((), ()))
F32 = jnp.float32
BF16 = jnp.bfloat16
MIB = 1024 * 1024


def identity(n):
    row = lax.broadcasted_iota(jnp.int32, (n, n), 0)
    col = lax.broadcasted_iota(jnp.int32, (n, n), 1)
    return jnp.where(row == col, 1.0, 0.0).astype(BF16)


def flipped(eye, block):
    return lax.dot_general(eye, block, NT, preferred_element_type=F32)


def gate_kernel(gated_ref, og_ref, taps_ref, skip_ref, out_ref, og_out_ref, skip_out_ref, rows_ref, og_rows_ref):
    skip_out_ref[...] = skip_ref[...]
    tokens, channels = gated_ref.shape
    count = tokens // 128
    pitch = og_rows_ref.shape[0] // count
    chunk = 34
    peers = out_ref.shape[0] // chunk
    per_peer = channels // peers
    eye = identity(channels)
    turned = flipped(eye, taps_ref[...])
    wide = (2 * count + 8) * pitch
    for r in range(2):
        rows_ref[pl.ds(wide + r * (peers + 8), peers), :] = jnp.concatenate(
            [turned[2 * r * peers:(2 * r + 1) * peers], turned[(2 * r + 1) * peers:(2 * r + 2) * peers]], axis=1
        )
    front = 8 * pitch
    for b in range(0, count, 2):
        turned = flipped(eye, gated_ref[pl.ds(b * 128, 256), :])
        for n in range(2):
            rows_ref[pl.ds(front + (b + n) * pitch, channels), :] = turned[:, n * 128:(n + 1) * 128]
        turned = flipped(eye, og_ref[pl.ds(b * 128, 256), :])
        for n in range(2):
            og_rows_ref[pl.ds((b + n) * pitch, channels), :] = turned[:, n * 128:(n + 1) * 128]
    sub = lax.broadcasted_iota(jnp.int32, (8, 128), 0)

    def tile(first):
        runs = []
        row = first
        while row < first + 8:
            j, r = divmod(row, chunk)
            at = row - first
            if r < 32:
                q, b = divmod(r, count)
                base = front + q * peers + j + (b - at) * pitch
                runs.append((at, rows_ref[pl.ds(base, 8, stride=pitch), :]))
                row += count - b
            else:
                base = wide + j + (r - 32 - at) * (peers + 8)
                runs.append((at, rows_ref[pl.ds(base, 8, stride=peers + 8), :]))
                row += 34 - r
        value = runs[0][1]
        for at, more in runs[1:]:
            value = jnp.where(sub >= at, more, value)
        return value

    for n in range(peers * chunk // 16):
        out_ref[pl.ds(n * 16, 16), :] = jnp.concatenate([tile(n * 16), tile(n * 16 + 8)], axis=0).astype(BF16)
    for j in range(peers):
        got = [og_rows_ref[pl.ds(q * peers + j, count, stride=pitch), :] for q in range(per_peer)]
        og_out_ref[pl.ds(j * 32, 32), :] = jnp.concatenate(got, axis=0).astype(BF16)


def conv_kernel(skip_ref, x_ref, out_ref, flat_ref, taps_ref, even_ref, odd_ref, steep_ref, shift_ref, wide_ref, out_rows):
    chunk = 34
    sources = x_ref.shape[0] // chunk
    per_peer = 4
    per_seg = sources // SEGS
    positions = per_seg * 4
    rows = positions * SEGS
    pitch = flat_ref.shape[0] // SEGS
    for g in range(SEGS):
        flat_ref[pl.ds(g * pitch, per_seg * chunk), :] = x_ref[pl.ds(g * per_seg * chunk, per_seg * chunk), :].astype(F32)
    low = lax.broadcasted_iota(jnp.int32, (4, 128), 1) < 64
    for r in range(2):
        for g in range(SEGS):
            even = flat_ref[pl.ds(g * pitch + 32 + r, 4, stride=2 * chunk), :]
            odd = flat_ref[pl.ds(g * pitch + chunk + 32 + r, 4, stride=2 * chunk), :]
            taps_ref[2 * r, pl.ds(4 * g, 4), :] = jnp.where(low, even, pltpu.roll(odd, 64, 1))
            taps_ref[2 * r + 1, pl.ds(4 * g, 4), :] = jnp.where(low, pltpu.roll(even, 64, 1), odd)
    lane = lax.broadcasted_iota(jnp.int32, (16, 128), 1)
    sub = lax.broadcasted_iota(jnp.int32, (16, 128), 0)
    first = lax.broadcasted_iota(jnp.int32, (8, 128), 0) == 0
    src = lax.broadcasted_iota(jnp.int32, (256, 256), 0)
    dst = lax.broadcasted_iota(jnp.int32, (256, 256), 1)
    for i in range(ROLLED, 8, 2):
        moved = jnp.where(dst < 128, 128 + dst - 16 * i, dst - 16 * (i + 1))
        shift_ref[(i - ROLLED) // 2] = jnp.where(src == moved, 1.0, 0.0).astype(BF16)
    for q in range(per_peer):
        wide_ref[q, 0] = jnp.zeros((128, 128), BF16)
        wide_ref[q, 34] = jnp.zeros((128, 128), BF16)

    for q in range(per_peer):
        none = jnp.zeros((16, 128), BF16)
        steep_ref[q, 0] = none
        rolled = none
        before = [none] * ROLLED
        for j in range(33):
            if j < 32:
                line = jnp.broadcast_to(taps_ref[q, pl.ds(j, 1), :], (16, 128))
                turned = pltpu.roll(line, 0, 1, stride=1, stride_axis=0).astype(BF16)
            else:
                turned = none
            strip = jnp.where(lane >= sub, turned, rolled)
            rolled = turned
            steep_ref[q, j + 1] = strip
            wide_ref[q, j + 1, pl.ds(0, 16), :] = strip
            for i in range(1, ROLLED):
                now = pltpu.roll(strip, 16 * i, 1)
                wide_ref[q, j + 1, pl.ds(16 * i, 16), :] = jnp.where(lane >= 16 * i, now, before[i])
                before[i] = now
        lhs = jnp.concatenate(
            [steep_ref[q, 0:33].reshape(33 * 16, 128), steep_ref[q, 1:34].reshape(33 * 16, 128)], axis=1
        )
        for i in range(ROLLED, 8, 2):
            moved = jnp.dot(lhs, shift_ref[(i - ROLLED) // 2], preferred_element_type=F32).astype(BF16)
            for n in range(2):
                wide_ref[q, 1:34, pl.ds(16 * (i + n), 16), :] = moved[:, 128 * n:128 * n + 128].reshape(33, 16, 128)
        for h in range(2):
            tiles = []
            for p in range(positions):
                start = (p // 4) * chunk + q * 8 + (p % 4) * 2 + h
                tiles.append(flat_ref[pl.ds(start, 8, stride=pitch), :])
            line = [jnp.where(first, 0.0, pltpu.roll(tiles[p + positions - LAGS], 1, 0)) for p in range(LAGS)] + tiles
            for a in range(len(line) // 2):
                even_ref[q, h, pl.ds(16 * a, 16), :] = jnp.concatenate([line[2 * a], line[2 * a + 1]], axis=0).astype(BF16)
            for a in range(len(line) // 2 - 1):
                odd_ref[q, h, pl.ds(16 * a, 16), :] = jnp.concatenate([line[2 * a + 1], line[2 * a + 2]], axis=0).astype(BF16)
        acc = None
        for s in range(LAGS + 1):
            start = LAGS - s
            if start % 2 == 0:
                lhs = [even_ref[q, h, pl.ds(start * 8, rows), :] for h in range(2)]
            else:
                lhs = [odd_ref[q, h, pl.ds((start - 1) * 8, rows), :] for h in range(2)]
            lhs = jnp.concatenate(lhs, axis=1)
            t = 2 * s
            rhs = jnp.concatenate(
                [
                    jnp.concatenate([wide_ref[q, t + 1], wide_ref[q, t + 2]], axis=1),
                    jnp.concatenate([wide_ref[q, t], wide_ref[q, t + 1]], axis=1),
                ],
                axis=0,
            )
            term = jnp.dot(lhs, rhs, preferred_element_type=F32)
            acc = term if acc is None else acc + term
        mine = lax.broadcasted_iota(jnp.int32, (2, 128), 0) * 128 + lax.broadcasted_iota(jnp.int32, (2, 128), 1)
        mine = jnp.where(mine == q * sources + lax.axis_index("seq"), skip_ref[...], 0.0)
        skip = jnp.sum(jnp.sum(mine, axis=1, keepdims=True), axis=0, keepdims=True)
        for p in range(positions):
            for h in range(2):
                start = (p // 4) * chunk + q * 8 + (p % 4) * 2 + h
                own = flat_ref[pl.ds(start, 8, stride=pitch), :]
                out_rows[q, pl.ds((p * 2 + h) * 8, 8), :] = acc[8 * p:8 * p + 8, h * 128:(h + 1) * 128] + skip * own
    for j in range(sources):
        g, jj = divmod(j, per_seg)
        got = [out_rows[q, pl.ds(jj * 64 + g, 8, stride=8), :] for q in range(per_peer)]
        out_ref[pl.ds(j * 32, 32), :] = jnp.concatenate(got, axis=0).astype(BF16)


def square_kernel(conv_ref, og_ref, square_ref):
    def step(n, total):
        part = pl.ds(pl.multiple_of(n * 128, 128), 128)
        mixed = conv_ref[part, :].astype(F32) * og_ref[part, :].astype(F32)
        return total + (mixed * mixed).reshape(8, 16, 128)

    total = lax.fori_loop(0, conv_ref.shape[0] // 128, step, jnp.zeros((8, 16, 128), F32), unroll=True)
    total = jnp.sum(total, axis=0)
    square_ref[...] = total[:8] + total[8:]


def mix_kernel(conv_ref, og_ref, mixed_ref, rows_ref):
    peers = conv_ref.shape[0] // 32
    count, channels, _ = mixed_ref.shape
    per_peer = channels // peers
    for j in range(peers):
        part = pl.ds(j * 32, 32)
        rows_ref[pl.ds(j * 40, 32), :] = conv_ref[part, :].astype(F32) * og_ref[part, :].astype(F32)
    for b in range(count):
        for q in range(per_peer):
            mixed_ref[b, pl.ds(q * peers, peers), :] = rows_ref[pl.ds(q * count + b, peers, stride=40), :]


def norm_kernel(mixed_ref, own_ref, first_ref, second_ref, third_ref, out_hbm, out_ref, sems):
    count = mixed_ref.shape[0]
    power = (own_ref[...] + first_ref[...] + second_ref[...] + third_ref[...]) * (1.0 / CH)
    scale = 1.0 / jnp.sqrt(power + 1e-05)
    eye = identity(128)
    copies = []
    for b in range(count):
        part = pl.ds(b * 128, 128)
        scaled = (mixed_ref[b] * scale[b:b + 1, :]).astype(BF16)
        out_ref[part, :] = flipped(eye, scaled).astype(BF16)
        copies.append(pltpu.make_async_copy(out_ref.at[part], out_hbm.at[part], sems.at[b]))
        copies[-1].start()
    for copy in copies:
        copy.wait()


def shape(dims, dtype):
    return jax.ShapeDtypeStruct(dims, dtype)


VMEM = pl.BlockSpec(memory_space=pltpu.VMEM)
SMEM = pl.BlockSpec(memory_space=pltpu.SMEM)
HBM = pl.BlockSpec(memory_space=pltpu.HBM)


def params(mib):
    return pltpu.CompilerParams(vmem_limit_bytes=mib * MIB)


def local(gate_in, value_in, out_gate, filter_taps, skip_gain):
    tokens, channels = gate_in.shape
    peers = lax.axis_size("seq")
    per_peer = channels // peers
    count = tokens // 128
    rows = peers * per_peer * count
    gated = (gate_in.astype(F32) * value_in.astype(F32)).astype(BF16)
    message, turned, skip = pl.pallas_call(
        gate_kernel,
        out_shape=(shape((peers * 34, 128), BF16), shape((rows, 128), BF16), shape((channels // 128, 128), F32)),
        in_specs=[VMEM] * 4,
        out_specs=(VMEM,) * 3,
        scratch_shapes=[
            pltpu.VMEM(((2 * count + 8) * (channels + 8) + 16 * (peers + 8), 128), F32),
            pltpu.VMEM((count * (channels + 8), 128), F32),
        ],
        compiler_params=params(12),
        name="gate",
    )(gated, out_gate, filter_taps, skip_gain.reshape(channels // 128, 128))
    message = lax.all_to_all(message.reshape(peers, 17, 2, 128), "seq", split_axis=0, concat_axis=0, tiled=True)
    convolved = pl.pallas_call(
        conv_kernel,
        out_shape=shape((rows, 128), BF16),
        in_specs=[VMEM, VMEM],
        out_specs=VMEM,
        scratch_shapes=[
            pltpu.VMEM((SEGS * 276, 128), F32),
            pltpu.VMEM((4, 32, 128), F32),
            pltpu.VMEM((4, 2, 384, 128), BF16),
            pltpu.VMEM((4, 2, 384, 128), BF16),
            pltpu.VMEM((4, 34, 16, 128), BF16),
            pltpu.VMEM((4, 256, 256), BF16),
            pltpu.VMEM((4, 35, 128, 128), BF16),
            pltpu.VMEM((4, 512, 128), F32),
        ],
        compiler_params=params(24),
        name="conv",
    )(skip, message.reshape(peers * 34, 128))
    convolved = lax.all_to_all(
        convolved.reshape(peers, 32, 128), "seq", split_axis=0, concat_axis=0, tiled=True
    ).reshape(rows, 128)
    squares = pl.pallas_call(
        square_kernel,
        out_shape=shape((count, 128), F32),
        in_specs=[VMEM] * 2,
        out_specs=VMEM,
        compiler_params=params(8),
        name="square",
    )(convolved, turned)
    group = lax.axis_size("mp")
    others = [lax.ppermute(squares, "mp", [(i, (i + k) % group) for i in range(group)]) for k in range(1, group)]
    mixed = pl.pallas_call(
        mix_kernel,
        out_shape=shape((count, channels, 128), F32),
        in_specs=[VMEM] * 2,
        out_specs=VMEM,
        scratch_shapes=[pltpu.VMEM((peers * 40, 128), F32)],
        compiler_params=params(8),
        cost_estimate=pl.CostEstimate(flops=20000000, bytes_accessed=8 * tokens * channels, transcendentals=0),
        name="mix",
    )(convolved, turned)
    return pl.pallas_call(
        norm_kernel,
        out_shape=shape((tokens, channels), BF16),
        in_specs=[VMEM] * 5,
        out_specs=HBM,
        scratch_shapes=[pltpu.VMEM((tokens, channels), BF16), pltpu.SemaphoreType.DMA((count,))],
        compiler_params=params(8),
        name="norm",
    )(mixed, squares, *others)


def solution(mesh):
    return jax.shard_map(
        local,
        mesh=mesh,
        in_specs=(P("seq", "mp"), P("seq", "mp"), P("seq", "mp"), P("seq", "mp"), P("mp")),
        out_specs=P("seq", "mp"),
        check_vma=False,
    )
```

```python
import jax
import jax.numpy as jnp
from jax import lax
from jax.experimental import pallas as pl
from jax.experimental.pallas import tpu as pltpu
from jax.sharding import PartitionSpec as P

CH = 1024
TAPS = 4096
BLOCK = 256
LAGS = TAPS // BLOCK
SEGS = 8
ROLLED = 6
NT = (((1,), (1,)), ((), ()))
F32 = jnp.float32
BF16 = jnp.bfloat16
MIB = 1024 * 1024


def identity(n):
    row = lax.broadcasted_iota(jnp.int32, (n, n), 0)
    col = lax.broadcasted_iota(jnp.int32, (n, n), 1)
    return jnp.where(row == col, 1.0, 0.0).astype(BF16)


def flipped(eye, block):
    return lax.dot_general(eye, block, NT, preferred_element_type=F32)


def gate_kernel(gate_hbm, value_hbm, og_hbm, taps_hbm, skip_hbm, out_ref, og_out_ref, skip_out_ref,
                gate_ref, value_ref, og_ref, taps_ref, rows_ref, og_rows_ref, sems):
    tokens, channels = gate_ref.shape
    count = tokens // 128
    pitch = og_rows_ref.shape[0] // count
    chunk = 34
    peers = out_ref.shape[0] // chunk
    per_peer = channels // peers
    step = 1024
    fetch = []
    for k in range(tokens // step):
        part = pl.ds(k * step, step)
        fetch.append([
            pltpu.make_async_copy(src.at[part], dst.at[part], sems.at[n, k])
            for n, (src, dst) in enumerate(((gate_hbm, gate_ref), (value_hbm, value_ref)))
        ])
    rest = [
        pltpu.make_async_copy(taps_hbm, taps_ref, sems.at[2, 0]),
        pltpu.make_async_copy(og_hbm, og_ref, sems.at[2, 1]),
        pltpu.make_async_copy(skip_hbm, skip_out_ref, sems.at[2, 2]),
    ]
    for copy in rest + [c for pair in fetch for c in pair]:
        copy.start()
    eye = identity(channels)
    front = 8 * pitch
    wide = (2 * count + 8) * pitch
    for copy in rest:
        copy.wait()
    turned = flipped(eye, taps_ref[...])
    for r in range(2):
        rows_ref[pl.ds(wide + r * (peers + 8), peers), :] = jnp.concatenate(
            [turned[2 * r * peers:(2 * r + 1) * peers], turned[(2 * r + 1) * peers:(2 * r + 2) * peers]], axis=1
        )
    for b in range(0, count, 2):
        turned = flipped(eye, og_ref[pl.ds(b * 128, 256), :])
        for n in range(2):
            og_rows_ref[pl.ds((b + n) * pitch, channels), :] = turned[:, n * 128:(n + 1) * 128]
    for j in range(peers):
        got = [og_rows_ref[pl.ds(q * peers + j, count, stride=pitch), :] for q in range(per_peer)]
        og_out_ref[pl.ds(j * 32, 32), :] = jnp.concatenate(got, axis=0).astype(BF16)
    for k, pair in enumerate(fetch):
        for copy in pair:
            copy.wait()
        part = pl.ds(k * step, step)
        gated = (gate_ref[part, :].astype(F32) * value_ref[part, :].astype(F32)).astype(BF16)
        for m in range(step // 256):
            turned = flipped(eye, gated[m * 256:(m + 1) * 256])
            for n in range(2):
                rows_ref[pl.ds(front + ((step // 128) * k + 2 * m + n) * pitch, channels), :] = turned[:, n * 128:(n + 1) * 128]
    sub = lax.broadcasted_iota(jnp.int32, (8, 128), 0)

    def tile(first):
        runs = []
        row = first
        while row < first + 8:
            j, r = divmod(row, chunk)
            at = row - first
            if r < 32:
                q, b = divmod(r, count)
                base = front + q * peers + j + (b - at) * pitch
                runs.append((at, rows_ref[pl.ds(base, 8, stride=pitch), :]))
                row += count - b
            else:
                base = wide + j + (r - 32 - at) * (peers + 8)
                runs.append((at, rows_ref[pl.ds(base, 8, stride=peers + 8), :]))
                row += 34 - r
        value = runs[0][1]
        for at, more in runs[1:]:
            value = jnp.where(sub >= at, more, value)
        return value

    for n in range(peers * chunk // 16):
        out_ref[pl.ds(n * 16, 16), :] = jnp.concatenate([tile(n * 16), tile(n * 16 + 8)], axis=0).astype(BF16)


def conv_kernel(skip_ref, x_ref, out_ref, flat_ref, taps_ref, even_ref, odd_ref, steep_ref, shift_ref, wide_ref, out_rows):
    chunk = 34
    sources = x_ref.shape[0] // chunk
    per_peer = 4
    per_seg = sources // SEGS
    positions = per_seg * 4
    rows = positions * SEGS
    pitch = flat_ref.shape[0] // SEGS
    for g in range(SEGS):
        flat_ref[pl.ds(g * pitch, per_seg * chunk), :] = x_ref[pl.ds(g * per_seg * chunk, per_seg * chunk), :].astype(F32)
    low = lax.broadcasted_iota(jnp.int32, (4, 128), 1) < 64
    for r in range(2):
        for g in range(SEGS):
            even = flat_ref[pl.ds(g * pitch + 32 + r, 4, stride=2 * chunk), :]
            odd = flat_ref[pl.ds(g * pitch + chunk + 32 + r, 4, stride=2 * chunk), :]
            taps_ref[2 * r, pl.ds(4 * g, 4), :] = jnp.where(low, even, pltpu.roll(odd, 64, 1))
            taps_ref[2 * r + 1, pl.ds(4 * g, 4), :] = jnp.where(low, pltpu.roll(even, 64, 1), odd)
    lane = lax.broadcasted_iota(jnp.int32, (16, 128), 1)
    sub = lax.broadcasted_iota(jnp.int32, (16, 128), 0)
    first = lax.broadcasted_iota(jnp.int32, (8, 128), 0) == 0
    src = lax.broadcasted_iota(jnp.int32, (256, 256), 0)
    dst = lax.broadcasted_iota(jnp.int32, (256, 256), 1)
    for i in range(ROLLED, 8, 2):
        moved = jnp.where(dst < 128, 128 + dst - 16 * i, dst - 16 * (i + 1))
        shift_ref[(i - ROLLED) // 2] = jnp.where(src == moved, 1.0, 0.0).astype(BF16)
    for q in range(per_peer):
        wide_ref[q, 0] = jnp.zeros((128, 128), BF16)
        wide_ref[q, 34] = jnp.zeros((128, 128), BF16)

    for q in range(per_peer):
        none = jnp.zeros((16, 128), BF16)
        steep_ref[q, 0] = none
        rolled = none
        before = [none] * ROLLED
        for j in range(33):
            if j < 32:
                line = jnp.broadcast_to(taps_ref[q, pl.ds(j, 1), :], (16, 128))
                turned = pltpu.roll(line, 0, 1, stride=1, stride_axis=0).astype(BF16)
            else:
                turned = none
            strip = jnp.where(lane >= sub, turned, rolled)
            rolled = turned
            steep_ref[q, j + 1] = strip
            wide_ref[q, j + 1, pl.ds(0, 16), :] = strip
            for i in range(1, ROLLED):
                now = pltpu.roll(strip, 16 * i, 1)
                wide_ref[q, j + 1, pl.ds(16 * i, 16), :] = jnp.where(lane >= 16 * i, now, before[i])
                before[i] = now
        lhs = jnp.concatenate(
            [steep_ref[q, 0:33].reshape(33 * 16, 128), steep_ref[q, 1:34].reshape(33 * 16, 128)], axis=1
        )
        for i in range(ROLLED, 8, 2):
            moved = jnp.dot(lhs, shift_ref[(i - ROLLED) // 2], preferred_element_type=F32).astype(BF16)
            for n in range(2):
                wide_ref[q, 1:34, pl.ds(16 * (i + n), 16), :] = moved[:, 128 * n:128 * n + 128].reshape(33, 16, 128)
        for h in range(2):
            tiles = []
            for p in range(positions):
                start = (p // 4) * chunk + q * 8 + (p % 4) * 2 + h
                tiles.append(flat_ref[pl.ds(start, 8, stride=pitch), :])
            line = [jnp.where(first, 0.0, pltpu.roll(tiles[p + positions - LAGS], 1, 0)) for p in range(LAGS)] + tiles
            for a in range(len(line) // 2):
                even_ref[q, h, pl.ds(16 * a, 16), :] = jnp.concatenate([line[2 * a], line[2 * a + 1]], axis=0).astype(BF16)
            for a in range(len(line) // 2 - 1):
                odd_ref[q, h, pl.ds(16 * a, 16), :] = jnp.concatenate([line[2 * a + 1], line[2 * a + 2]], axis=0).astype(BF16)
        acc = None
        for s in range(LAGS + 1):
            start = LAGS - s
            if start % 2 == 0:
                lhs = [even_ref[q, h, pl.ds(start * 8, rows), :] for h in range(2)]
            else:
                lhs = [odd_ref[q, h, pl.ds((start - 1) * 8, rows), :] for h in range(2)]
            lhs = jnp.concatenate(lhs, axis=1)
            t = 2 * s
            rhs = jnp.concatenate(
                [
                    jnp.concatenate([wide_ref[q, t + 1], wide_ref[q, t + 2]], axis=1),
                    jnp.concatenate([wide_ref[q, t], wide_ref[q, t + 1]], axis=1),
                ],
                axis=0,
            )
            term = jnp.dot(lhs, rhs, preferred_element_type=F32)
            acc = term if acc is None else acc + term
        mine = lax.broadcasted_iota(jnp.int32, (2, 128), 0) * 128 + lax.broadcasted_iota(jnp.int32, (2, 128), 1)
        mine = jnp.where(mine == q * sources + lax.axis_index("seq"), skip_ref[...], 0.0)
        skip = jnp.sum(jnp.sum(mine, axis=1, keepdims=True), axis=0, keepdims=True)
        for p in range(positions):
            for h in range(2):
                start = (p // 4) * chunk + q * 8 + (p % 4) * 2 + h
                own = flat_ref[pl.ds(start, 8, stride=pitch), :]
                out_rows[q, pl.ds((p * 2 + h) * 8, 8), :] = acc[8 * p:8 * p + 8, h * 128:(h + 1) * 128] + skip * own
    for j in range(sources):
        g, jj = divmod(j, per_seg)
        got = [out_rows[q, pl.ds(jj * 64 + g, 8, stride=8), :] for q in range(per_peer)]
        out_ref[pl.ds(j * 32, 32), :] = jnp.concatenate(got, axis=0).astype(BF16)


def square_kernel(conv_ref, og_ref, square_ref):
    def step(n, total):
        part = pl.ds(pl.multiple_of(n * 128, 128), 128)
        mixed = conv_ref[part, :].astype(F32) * og_ref[part, :].astype(F32)
        return total + (mixed * mixed).reshape(8, 16, 128)

    total = lax.fori_loop(0, conv_ref.shape[0] // 128, step, jnp.zeros((8, 16, 128), F32), unroll=True)
    total = jnp.sum(total, axis=0)
    square_ref[...] = total[:8] + total[8:]


def mix_kernel(conv_ref, og_ref, mixed_ref, rows_ref):
    peers = conv_ref.shape[0] // 32
    count, channels, _ = mixed_ref.shape
    per_peer = channels // peers
    for j in range(peers):
        part = pl.ds(j * 32, 32)
        rows_ref[pl.ds(j * 40, 32), :] = conv_ref[part, :].astype(F32) * og_ref[part, :].astype(F32)
    for b in range(count):
        for q in range(per_peer):
            mixed_ref[b, pl.ds(q * peers, peers), :] = rows_ref[pl.ds(q * count + b, peers, stride=40), :]


def norm_kernel(mixed_ref, own_ref, first_ref, second_ref, third_ref, out_hbm, out_ref, sems):
    count = mixed_ref.shape[0]
    power = (own_ref[...] + first_ref[...] + second_ref[...] + third_ref[...]) * (1.0 / CH)
    scale = 1.0 / jnp.sqrt(power + 1e-05)
    eye = identity(128)
    copies = []
    for b in range(count):
        part = pl.ds(b * 128, 128)
        scaled = (mixed_ref[b] * scale[b:b + 1, :]).astype(BF16)
        out_ref[part, :] = flipped(eye, scaled).astype(BF16)
        copies.append(pltpu.make_async_copy(out_ref.at[part], out_hbm.at[part], sems.at[b]))
        copies[-1].start()
    for copy in copies:
        copy.wait()


def shape(dims, dtype):
    return jax.ShapeDtypeStruct(dims, dtype)


VMEM = pl.BlockSpec(memory_space=pltpu.VMEM)
SMEM = pl.BlockSpec(memory_space=pltpu.SMEM)
HBM = pl.BlockSpec(memory_space=pltpu.HBM)


def params(mib):
    return pltpu.CompilerParams(vmem_limit_bytes=mib * MIB)


def local(gate_in, value_in, out_gate, filter_taps, skip_gain):
    tokens, channels = gate_in.shape
    peers = lax.axis_size("seq")
    per_peer = channels // peers
    count = tokens // 128
    rows = peers * per_peer * count
    inputs = (gate_in, value_in, out_gate, filter_taps, skip_gain.reshape(channels // 128, 128))
    message, turned, skip = pl.pallas_call(
        gate_kernel,
        out_shape=(shape((peers * 34, 128), BF16), shape((rows, 128), BF16), shape((channels // 128, 128), F32)),
        in_specs=[HBM] * 5,
        out_specs=(VMEM,) * 3,
        scratch_shapes=[
            pltpu.VMEM((tokens, channels), BF16),
            pltpu.VMEM((tokens, channels), BF16),
            pltpu.VMEM((tokens, channels), BF16),
            pltpu.VMEM(filter_taps.shape, BF16),
            pltpu.VMEM(((2 * count + 8) * (channels + 8) + 16 * (peers + 8), 128), F32),
            pltpu.VMEM((count * (channels + 8), 128), F32),
            pltpu.SemaphoreType.DMA((3, tokens // 256)),
        ],
        compiler_params=params(16),
        name="gate",
    )(*(pltpu.with_memory_space_constraint(a, pltpu.HBM) for a in inputs))
    message = lax.all_to_all(message.reshape(peers, 17, 2, 128), "seq", split_axis=0, concat_axis=0, tiled=True)
    convolved = pl.pallas_call(
        conv_kernel,
        out_shape=shape((rows, 128), BF16),
        in_specs=[VMEM, VMEM],
        out_specs=VMEM,
        scratch_shapes=[
            pltpu.VMEM((SEGS * 276, 128), F32),
            pltpu.VMEM((4, 32, 128), F32),
            pltpu.VMEM((4, 2, 384, 128), BF16),
            pltpu.VMEM((4, 2, 384, 128), BF16),
            pltpu.VMEM((4, 34, 16, 128), BF16),
            pltpu.VMEM((4, 256, 256), BF16),
            pltpu.VMEM((4, 35, 128, 128), BF16),
            pltpu.VMEM((4, 512, 128), F32),
        ],
        compiler_params=params(24),
        name="conv",
    )(skip, message.reshape(peers * 34, 128))
    convolved = lax.all_to_all(
        convolved.reshape(peers, 32, 128), "seq", split_axis=0, concat_axis=0, tiled=True
    ).reshape(rows, 128)
    squares = pl.pallas_call(
        square_kernel,
        out_shape=shape((count, 128), F32),
        in_specs=[VMEM] * 2,
        out_specs=VMEM,
        compiler_params=params(8),
        name="square",
    )(convolved, turned)
    group = lax.axis_size("mp")
    others = [lax.ppermute(squares, "mp", [(i, (i + k) % group) for i in range(group)]) for k in range(1, group)]
    mixed = pl.pallas_call(
        mix_kernel,
        out_shape=shape((count, channels, 128), F32),
        in_specs=[VMEM] * 2,
        out_specs=VMEM,
        scratch_shapes=[pltpu.VMEM((peers * 40, 128), F32)],
        compiler_params=params(8),
        cost_estimate=pl.CostEstimate(flops=20000000, bytes_accessed=8 * tokens * channels, transcendentals=0),
        name="mix",
    )(convolved, turned)
    return pl.pallas_call(
        norm_kernel,
        out_shape=shape((tokens, channels), BF16),
        in_specs=[VMEM] * 5,
        out_specs=HBM,
        scratch_shapes=[pltpu.VMEM((tokens, channels), BF16), pltpu.SemaphoreType.DMA((count,))],
        compiler_params=params(8),
        name="norm",
    )(mixed, squares, *others)


def solution(mesh):
    return jax.shard_map(
        local,
        mesh=mesh,
        in_specs=(P("seq", "mp"), P("seq", "mp"), P("seq", "mp"), P("seq", "mp"), P("mp")),
        out_specs=P("seq", "mp"),
        check_vma=False,
    )
```

```python
import jax
import jax.numpy as jnp
from jax import lax
from jax.experimental import pallas as pl
from jax.experimental.pallas import tpu as pltpu
from jax.sharding import PartitionSpec as P

CH = 1024
TAPS = 4096
BLOCK = 256
LAGS = TAPS // BLOCK
SEGS = 8
STAGGER = 8000
ROLLED = 6
NT = (((1,), (1,)), ((), ()))
F32 = jnp.float32
BF16 = jnp.bfloat16
MIB = 1024 * 1024


def identity(n):
    row = lax.broadcasted_iota(jnp.int32, (n, n), 0)
    col = lax.broadcasted_iota(jnp.int32, (n, n), 1)
    return jnp.where(row == col, 1.0, 0.0).astype(BF16)


def flipped(eye, block):
    return lax.dot_general(eye, block, NT, preferred_element_type=F32)


def gate_kernel(gate_hbm, value_hbm, taps_hbm, skip_hbm, og_hbm, out_ref, skip_out_ref, og_ref,
                gate_ref, value_ref, taps_ref, rows_ref, sems):
    tokens, channels = gate_ref.shape
    count = tokens // 128
    pitch = channels + 8
    chunk = 34
    peers = out_ref.shape[0] // chunk
    per_peer = channels // peers
    step = 1024
    fetch = []
    for k in range(tokens // step):
        part = pl.ds(k * step, step)
        fetch.append([
            pltpu.make_async_copy(src.at[part], dst.at[part], sems.at[n, k])
            for n, (src, dst) in enumerate(((gate_hbm, gate_ref), (value_hbm, value_ref)))
        ])
    rest = [
        pltpu.make_async_copy(taps_hbm, taps_ref, sems.at[2, 0]),
        pltpu.make_async_copy(og_hbm, og_ref, sems.at[2, 1]),
        pltpu.make_async_copy(skip_hbm, skip_out_ref, sems.at[2, 2]),
    ]
    for copy in rest[:1] + [c for pair in fetch for c in pair] + rest[1:]:
        copy.start()
    eye = identity(channels)
    front = 8 * pitch
    wide = (2 * count + 8) * pitch
    rest[0].wait()
    turned = flipped(eye, taps_ref[...])
    for r in range(2):
        rows_ref[pl.ds(wide + r * (peers + 8), peers), :] = jnp.concatenate(
            [turned[2 * r * peers:(2 * r + 1) * peers], turned[(2 * r + 1) * peers:(2 * r + 2) * peers]], axis=1
        )
    for k, pair in enumerate(fetch):
        for copy in pair:
            copy.wait()
        part = pl.ds(k * step, step)
        gated = (gate_ref[part, :].astype(F32) * value_ref[part, :].astype(F32)).astype(BF16)
        for m in range(step // 256):
            turned = flipped(eye, gated[m * 256:(m + 1) * 256])
            for n in range(2):
                rows_ref[pl.ds(front + ((step // 128) * k + 2 * m + n) * pitch, channels), :] = turned[:, n * 128:(n + 1) * 128]
    sub = lax.broadcasted_iota(jnp.int32, (8, 128), 0)

    def tile(first):
        runs = []
        row = first
        while row < first + 8:
            j, r = divmod(row, chunk)
            at = row - first
            if r < 32:
                q, b = divmod(r, count)
                base = front + q * peers + j + (b - at) * pitch
                runs.append((at, rows_ref[pl.ds(base, 8, stride=pitch), :]))
                row += count - b
            else:
                base = wide + j + (r - 32 - at) * (peers + 8)
                runs.append((at, rows_ref[pl.ds(base, 8, stride=peers + 8), :]))
                row += 34 - r
        value = runs[0][1]
        for at, more in runs[1:]:
            value = jnp.where(sub >= at, more, value)
        return value

    for n in range(peers * chunk // 16):
        out_ref[pl.ds(n * 16, 16), :] = jnp.concatenate([tile(n * 16), tile(n * 16 + 8)], axis=0).astype(BF16)
    for copy in rest[1:]:
        copy.wait()

    @pl.when(lax.rem(lax.axis_index("mp"), 2) == 1)
    def _():
        pl.delay(STAGGER)


def conv_kernel(skip_ref, x_ref, og_ref, out_ref, og_out_ref, og_rows_ref, flat_ref, taps_ref, even_ref, odd_ref, steep_ref, shift_ref, wide_ref, out_rows):
    chunk = 34
    sources = x_ref.shape[0] // chunk
    per_peer = 4
    per_seg = sources // SEGS
    positions = per_seg * 4
    rows = positions * SEGS
    pitch = flat_ref.shape[0] // SEGS
    for g in range(SEGS):
        flat_ref[pl.ds(g * pitch, per_seg * chunk), :] = x_ref[pl.ds(g * per_seg * chunk, per_seg * chunk), :].astype(F32)
    low = lax.broadcasted_iota(jnp.int32, (4, 128), 1) < 64
    for r in range(2):
        for g in range(SEGS):
            even = flat_ref[pl.ds(g * pitch + 32 + r, 4, stride=2 * chunk), :]
            odd = flat_ref[pl.ds(g * pitch + chunk + 32 + r, 4, stride=2 * chunk), :]
            taps_ref[2 * r, pl.ds(4 * g, 4), :] = jnp.where(low, even, pltpu.roll(odd, 64, 1))
            taps_ref[2 * r + 1, pl.ds(4 * g, 4), :] = jnp.where(low, pltpu.roll(even, 64, 1), odd)
    lane = lax.broadcasted_iota(jnp.int32, (16, 128), 1)
    sub = lax.broadcasted_iota(jnp.int32, (16, 128), 0)
    first = lax.broadcasted_iota(jnp.int32, (8, 128), 0) == 0
    src = lax.broadcasted_iota(jnp.int32, (256, 256), 0)
    dst = lax.broadcasted_iota(jnp.int32, (256, 256), 1)
    for i in range(ROLLED, 8, 2):
        moved = jnp.where(dst < 128, 128 + dst - 16 * i, dst - 16 * (i + 1))
        shift_ref[(i - ROLLED) // 2] = jnp.where(src == moved, 1.0, 0.0).astype(BF16)
    for q in range(per_peer):
        wide_ref[q, 0] = jnp.zeros((128, 128), BF16)
        wide_ref[q, 34] = jnp.zeros((128, 128), BF16)

    def toeplitz(q):
        none = jnp.zeros((16, 128), BF16)
        steep_ref[q, 0] = none
        rolled = none
        before = [none] * ROLLED
        for j in range(33):
            if j < 32:
                line = jnp.broadcast_to(taps_ref[q, pl.ds(j, 1), :], (16, 128))
                turned = pltpu.roll(line, 0, 1, stride=1, stride_axis=0).astype(BF16)
            else:
                turned = none
            strip = jnp.where(lane >= sub, turned, rolled)
            rolled = turned
            steep_ref[q, j + 1] = strip
            wide_ref[q, j + 1, pl.ds(0, 16), :] = strip
            for i in range(1, ROLLED):
                now = pltpu.roll(strip, 16 * i, 1)
                wide_ref[q, j + 1, pl.ds(16 * i, 16), :] = jnp.where(lane >= 16 * i, now, before[i])
                before[i] = now
        lhs = jnp.concatenate(
            [steep_ref[q, 0:33].reshape(33 * 16, 128), steep_ref[q, 1:34].reshape(33 * 16, 128)], axis=1
        )
        for i in range(ROLLED, 8, 2):
            moved = jnp.dot(lhs, shift_ref[(i - ROLLED) // 2], preferred_element_type=F32).astype(BF16)
            for n in range(2):
                wide_ref[q, 1:34, pl.ds(16 * (i + n), 16), :] = moved[:, 128 * n:128 * n + 128].reshape(33, 16, 128)

    def signal(q):
        for h in range(2):
            tiles = []
            for p in range(positions):
                start = (p // 4) * chunk + q * 8 + (p % 4) * 2 + h
                tiles.append(flat_ref[pl.ds(start, 8, stride=pitch), :])
            line = [jnp.where(first, 0.0, pltpu.roll(tiles[p + positions - LAGS], 1, 0)) for p in range(LAGS)] + tiles
            for a in range(len(line) // 2):
                even_ref[q, h, pl.ds(16 * a, 16), :] = jnp.concatenate([line[2 * a], line[2 * a + 1]], axis=0).astype(BF16)
            for a in range(len(line) // 2 - 1):
                odd_ref[q, h, pl.ds(16 * a, 16), :] = jnp.concatenate([line[2 * a + 1], line[2 * a + 2]], axis=0).astype(BF16)

    def multiply(q):
        acc = None
        for s in range(LAGS + 1):
            start = LAGS - s
            if start % 2 == 0:
                lhs = [even_ref[q, h, pl.ds(start * 8, rows), :] for h in range(2)]
            else:
                lhs = [odd_ref[q, h, pl.ds((start - 1) * 8, rows), :] for h in range(2)]
            lhs = jnp.concatenate(lhs, axis=1)
            t = 2 * s
            rhs = jnp.concatenate(
                [
                    jnp.concatenate([wide_ref[q, t + 1], wide_ref[q, t + 2]], axis=1),
                    jnp.concatenate([wide_ref[q, t], wide_ref[q, t + 1]], axis=1),
                ],
                axis=0,
            )
            term = jnp.dot(lhs, rhs, preferred_element_type=F32)
            acc = term if acc is None else acc + term
        mine = lax.broadcasted_iota(jnp.int32, (2, 128), 0) * 128 + lax.broadcasted_iota(jnp.int32, (2, 128), 1)
        mine = jnp.where(mine == q * sources + lax.axis_index("seq"), skip_ref[...], 0.0)
        skip = jnp.sum(jnp.sum(mine, axis=1, keepdims=True), axis=0, keepdims=True)
        for p in range(positions):
            for h in range(2):
                start = (p // 4) * chunk + q * 8 + (p % 4) * 2 + h
                own = flat_ref[pl.ds(start, 8, stride=pitch), :]
                out_rows[q, pl.ds((p * 2 + h) * 8, 8), :] = acc[8 * p:8 * p + 8, h * 128:(h + 1) * 128] + skip * own
    tokens, channels = og_ref.shape
    count = tokens // 128
    og_pitch = og_rows_ref.shape[0] // count
    eye = identity(channels)
    for b in range(0, count, 2):
        turned = flipped(eye, og_ref[pl.ds(b * 128, 256), :])
        for n in range(2):
            og_rows_ref[pl.ds((b + n) * og_pitch, channels), :] = turned[:, n * 128:(n + 1) * 128]

    def og_rows(first, last):
        for j in range(first, last):
            got = [og_rows_ref[pl.ds(q * sources + j, count, stride=og_pitch), :] for q in range(per_peer)]
            og_out_ref[pl.ds(j * 32, 32), :] = jnp.concatenate(got, axis=0).astype(BF16)

    toeplitz(0)
    signal(0)
    for q in range(per_peer):
        og_rows(q * sources // per_peer, (q + 1) * sources // per_peer)
        if q + 1 < per_peer:
            toeplitz(q + 1)
            signal(q + 1)
        multiply(q)

    for j in range(sources):
        g, jj = divmod(j, per_seg)
        got = [out_rows[q, pl.ds(jj * 64 + g, 8, stride=8), :] for q in range(per_peer)]
        out_ref[pl.ds(j * 32, 32), :] = jnp.concatenate(got, axis=0).astype(BF16)


def square_kernel(conv_ref, og_ref, square_ref):
    def step(n, total):
        part = pl.ds(pl.multiple_of(n * 128, 128), 128)
        mixed = conv_ref[part, :].astype(F32) * og_ref[part, :].astype(F32)
        return total + (mixed * mixed).reshape(8, 16, 128)

    total = lax.fori_loop(0, conv_ref.shape[0] // 128, step, jnp.zeros((8, 16, 128), F32), unroll=True)
    total = jnp.sum(total, axis=0)
    square_ref[...] = total[:8] + total[8:]


def mix_kernel(conv_ref, og_ref, mixed_ref, rows_ref):
    peers = conv_ref.shape[0] // 32
    count, channels, _ = mixed_ref.shape
    per_peer = channels // peers
    for j in range(peers):
        part = pl.ds(j * 32, 32)
        rows_ref[pl.ds(j * 40, 32), :] = conv_ref[part, :].astype(F32) * og_ref[part, :].astype(F32)
    for b in range(count):
        for q in range(per_peer):
            mixed_ref[b, pl.ds(q * peers, peers), :] = rows_ref[pl.ds(q * count + b, peers, stride=40), :]


def norm_kernel(mixed_ref, own_ref, first_ref, second_ref, third_ref, out_hbm, out_ref, sems):
    count = mixed_ref.shape[0]
    power = (own_ref[...] + first_ref[...] + second_ref[...] + third_ref[...]) * (1.0 / CH)
    scale = 1.0 / jnp.sqrt(power + 1e-05)
    eye = identity(128)
    copies = []
    for b in range(count):
        part = pl.ds(b * 128, 128)
        scaled = (mixed_ref[b] * scale[b:b + 1, :]).astype(BF16)
        out_ref[part, :] = flipped(eye, scaled).astype(BF16)
        copies.append(pltpu.make_async_copy(out_ref.at[part], out_hbm.at[part], sems.at[b]))
        copies[-1].start()
    for copy in copies:
        copy.wait()


def shape(dims, dtype):
    return jax.ShapeDtypeStruct(dims, dtype)


VMEM = pl.BlockSpec(memory_space=pltpu.VMEM)
SMEM = pl.BlockSpec(memory_space=pltpu.SMEM)
HBM = pl.BlockSpec(memory_space=pltpu.HBM)


def params(mib):
    return pltpu.CompilerParams(vmem_limit_bytes=mib * MIB)


def local(gate_in, value_in, out_gate, filter_taps, skip_gain):
    tokens, channels = gate_in.shape
    peers = lax.axis_size("seq")
    per_peer = channels // peers
    count = tokens // 128
    rows = peers * per_peer * count
    inputs = (gate_in, value_in, filter_taps, skip_gain.reshape(channels // 128, 128), out_gate)
    message, skip, og_here = pl.pallas_call(
        gate_kernel,
        out_shape=(shape((peers * 34, 128), BF16), shape((channels // 128, 128), F32), shape((tokens, channels), BF16)),
        in_specs=[HBM] * 5,
        out_specs=(VMEM,) * 3,
        scratch_shapes=[
            pltpu.VMEM((tokens, channels), BF16),
            pltpu.VMEM((tokens, channels), BF16),
            pltpu.VMEM(filter_taps.shape, BF16),
            pltpu.VMEM(((2 * count + 8) * (channels + 8) + 16 * (peers + 8), 128), F32),
            pltpu.SemaphoreType.DMA((3, tokens // 256)),
        ],
        compiler_params=params(16),
        name="gate",
    )(*(pltpu.with_memory_space_constraint(a, pltpu.HBM) for a in inputs))
    message = lax.all_to_all(message.reshape(peers, 17, 2, 128), "seq", split_axis=0, concat_axis=0, tiled=True)
    convolved, turned = pl.pallas_call(
        conv_kernel,
        out_shape=(shape((rows, 128), BF16), shape((rows, 128), BF16)),
        in_specs=[VMEM] * 3,
        out_specs=(VMEM, VMEM),
        scratch_shapes=[
            pltpu.VMEM((count * (channels + 8), 128), F32),
            pltpu.VMEM((SEGS * 276, 128), F32),
            pltpu.VMEM((4, 32, 128), F32),
            pltpu.VMEM((4, 2, 384, 128), BF16),
            pltpu.VMEM((4, 2, 384, 128), BF16),
            pltpu.VMEM((4, 34, 16, 128), BF16),
            pltpu.VMEM((4, 256, 256), BF16),
            pltpu.VMEM((4, 35, 128, 128), BF16),
            pltpu.VMEM((4, 512, 128), F32),
        ],
        compiler_params=params(24),
        name="conv",
    )(skip, message.reshape(peers * 34, 128), og_here)
    convolved = lax.all_to_all(
        convolved.reshape(peers, 32, 128), "seq", split_axis=0, concat_axis=0, tiled=True
    ).reshape(rows, 128)
    squares = pl.pallas_call(
        square_kernel,
        out_shape=shape((count, 128), F32),
        in_specs=[VMEM] * 2,
        out_specs=VMEM,
        compiler_params=params(8),
        name="square",
    )(convolved, turned)
    group = lax.axis_size("mp")
    others = [lax.ppermute(squares, "mp", [(i, (i + k) % group) for i in range(group)]) for k in range(1, group)]
    mixed = pl.pallas_call(
        mix_kernel,
        out_shape=shape((count, channels, 128), F32),
        in_specs=[VMEM] * 2,
        out_specs=VMEM,
        scratch_shapes=[pltpu.VMEM((peers * 40, 128), F32)],
        compiler_params=params(8),
        cost_estimate=pl.CostEstimate(flops=20000000, bytes_accessed=8 * tokens * channels, transcendentals=0),
        name="mix",
    )(convolved, turned)
    return pl.pallas_call(
        norm_kernel,
        out_shape=shape((tokens, channels), BF16),
        in_specs=[VMEM] * 5,
        out_specs=HBM,
        scratch_shapes=[pltpu.VMEM((tokens, channels), BF16), pltpu.SemaphoreType.DMA((count,))],
        compiler_params=params(8),
        name="norm",
    )(mixed, squares, *others)


def solution(mesh):
    return jax.shard_map(
        local,
        mesh=mesh,
        in_specs=(P("seq", "mp"), P("seq", "mp"), P("seq", "mp"), P("seq", "mp"), P("mp")),
        out_specs=P("seq", "mp"),
        check_vma=False,
    )
```

```python
import jax
import jax.numpy as jnp
from jax import lax
from jax.experimental import pallas as pl
from jax.experimental.pallas import tpu as pltpu
from jax.sharding import PartitionSpec as P

CH = 1024
TAPS = 4096
BLOCK = 256
LAGS = TAPS // BLOCK
SEGS = 8
STAGGER = 8000
ROLLED = (6, 6, 8, 8)
NT = (((1,), (1,)), ((), ()))
F32 = jnp.float32
BF16 = jnp.bfloat16
MIB = 1024 * 1024


def identity(n):
    row = lax.broadcasted_iota(jnp.int32, (n, n), 0)
    col = lax.broadcasted_iota(jnp.int32, (n, n), 1)
    return jnp.where(row == col, 1.0, 0.0).astype(BF16)


def flipped(eye, block):
    return lax.dot_general(eye, block, NT, preferred_element_type=F32)


def gate_kernel(gate_hbm, value_hbm, taps_hbm, skip_hbm, og_hbm, out_ref, skip_out_ref, og_ref,
                gate_ref, value_ref, taps_ref, rows_ref, sems):
    tokens, channels = gate_ref.shape
    count = tokens // 128
    pitch = channels + 8
    chunk = 34
    peers = out_ref.shape[0] // chunk
    per_peer = channels // peers
    step = 1024
    fetch = []
    for k in range(tokens // step):
        part = pl.ds(k * step, step)
        fetch.append([
            pltpu.make_async_copy(src.at[part], dst.at[part], sems.at[n, k])
            for n, (src, dst) in enumerate(((gate_hbm, gate_ref), (value_hbm, value_ref)))
        ])
    rest = [
        pltpu.make_async_copy(taps_hbm, taps_ref, sems.at[2, 0]),
        pltpu.make_async_copy(og_hbm, og_ref, sems.at[2, 1]),
        pltpu.make_async_copy(skip_hbm, skip_out_ref, sems.at[2, 2]),
    ]
    for copy in rest[:1] + [c for pair in fetch for c in pair] + rest[1:]:
        copy.start()
    eye = identity(channels)
    front = 8 * pitch
    wide = (2 * count + 8) * pitch
    rest[0].wait()
    turned = flipped(eye, taps_ref[...])
    for r in range(2):
        rows_ref[pl.ds(wide + r * (peers + 8), peers), :] = jnp.concatenate(
            [turned[2 * r * peers:(2 * r + 1) * peers], turned[(2 * r + 1) * peers:(2 * r + 2) * peers]], axis=1
        )
    for k, pair in enumerate(fetch):
        for copy in pair:
            copy.wait()
        part = pl.ds(k * step, step)
        gated = (gate_ref[part, :].astype(F32) * value_ref[part, :].astype(F32)).astype(BF16)
        for m in range(step // 256):
            turned = flipped(eye, gated[m * 256:(m + 1) * 256])
            for n in range(2):
                rows_ref[pl.ds(front + ((step // 128) * k + 2 * m + n) * pitch, channels), :] = turned[:, n * 128:(n + 1) * 128]
    sub = lax.broadcasted_iota(jnp.int32, (8, 128), 0)

    def tile(first):
        runs = []
        row = first
        while row < first + 8:
            j, r = divmod(row, chunk)
            at = row - first
            if r < 32:
                q, b = divmod(r, count)
                base = front + q * peers + j + (b - at) * pitch
                runs.append((at, rows_ref[pl.ds(base, 8, stride=pitch), :]))
                row += count - b
            else:
                base = wide + j + (r - 32 - at) * (peers + 8)
                runs.append((at, rows_ref[pl.ds(base, 8, stride=peers + 8), :]))
                row += 34 - r
        value = runs[0][1]
        for at, more in runs[1:]:
            value = jnp.where(sub >= at, more, value)
        return value

    for n in range(peers * chunk // 16):
        out_ref[pl.ds(n * 16, 16), :] = jnp.concatenate([tile(n * 16), tile(n * 16 + 8)], axis=0).astype(BF16)
    for copy in rest[1:]:
        copy.wait()

    @pl.when(lax.rem(lax.axis_index("mp"), 2) == 1)
    def _():
        pl.delay(STAGGER)


def conv_kernel(skip_ref, x_ref, og_ref, out_ref, og_out_ref, og_rows_ref, flat_ref, taps_ref, even_ref, odd_ref, steep_ref, shift_ref, wide_ref, out_rows):
    chunk = 34
    sources = x_ref.shape[0] // chunk
    per_peer = 4
    per_seg = sources // SEGS
    positions = per_seg * 4
    rows = positions * SEGS
    pitch = flat_ref.shape[0] // SEGS
    for g in range(SEGS):
        flat_ref[pl.ds(g * pitch, per_seg * chunk), :] = x_ref[pl.ds(g * per_seg * chunk, per_seg * chunk), :].astype(F32)
    low = lax.broadcasted_iota(jnp.int32, (4, 128), 1) < 64
    for r in range(2):
        for g in range(SEGS):
            even = flat_ref[pl.ds(g * pitch + 32 + r, 4, stride=2 * chunk), :]
            odd = flat_ref[pl.ds(g * pitch + chunk + 32 + r, 4, stride=2 * chunk), :]
            taps_ref[2 * r, pl.ds(4 * g, 4), :] = jnp.where(low, even, pltpu.roll(odd, 64, 1))
            taps_ref[2 * r + 1, pl.ds(4 * g, 4), :] = jnp.where(low, pltpu.roll(even, 64, 1), odd)
    lane = lax.broadcasted_iota(jnp.int32, (16, 128), 1)
    sub = lax.broadcasted_iota(jnp.int32, (16, 128), 0)
    first = lax.broadcasted_iota(jnp.int32, (8, 128), 0) == 0
    src = lax.broadcasted_iota(jnp.int32, (256, 256), 0)
    dst = lax.broadcasted_iota(jnp.int32, (256, 256), 1)
    for i in range(6, 8, 2):
        moved = jnp.where(dst < 128, 128 + dst - 16 * i, dst - 16 * (i + 1))
        shift_ref[(i - 6) // 2] = jnp.where(src == moved, 1.0, 0.0).astype(BF16)
    for q in range(per_peer):
        wide_ref[q, 0] = jnp.zeros((128, 128), BF16)
        wide_ref[q, 34] = jnp.zeros((128, 128), BF16)

    def toeplitz(q):
        rolls = ROLLED[q]
        none = jnp.zeros((16, 128), BF16)
        steep_ref[q, 0] = none
        rolled = none
        before = [none] * rolls
        for j in range(33):
            if j < 32:
                line = jnp.broadcast_to(taps_ref[q, pl.ds(j, 1), :], (16, 128))
                turned = pltpu.roll(line, 0, 1, stride=1, stride_axis=0).astype(BF16)
            else:
                turned = none
            strip = jnp.where(lane >= sub, turned, rolled)
            rolled = turned
            steep_ref[q, j + 1] = strip
            wide_ref[q, j + 1, pl.ds(0, 16), :] = strip
            for i in range(1, rolls):
                now = pltpu.roll(strip, 16 * i, 1)
                wide_ref[q, j + 1, pl.ds(16 * i, 16), :] = jnp.where(lane >= 16 * i, now, before[i])
                before[i] = now
        lhs = jnp.concatenate(
            [steep_ref[q, 0:33].reshape(33 * 16, 128), steep_ref[q, 1:34].reshape(33 * 16, 128)], axis=1
        )
        for i in range(rolls, 8, 2):
            moved = jnp.dot(lhs, shift_ref[(i - 6) // 2], preferred_element_type=F32).astype(BF16)
            for n in range(2):
                wide_ref[q, 1:34, pl.ds(16 * (i + n), 16), :] = moved[:, 128 * n:128 * n + 128].reshape(33, 16, 128)

    def signal(q):
        for h in range(2):
            tiles = []
            for p in range(positions):
                start = (p // 4) * chunk + q * 8 + (p % 4) * 2 + h
                tiles.append(flat_ref[pl.ds(start, 8, stride=pitch), :])
            line = [jnp.where(first, 0.0, pltpu.roll(tiles[p + positions - LAGS], 1, 0)) for p in range(LAGS)] + tiles
            for a in range(len(line) // 2):
                even_ref[q, h, pl.ds(16 * a, 16), :] = jnp.concatenate([line[2 * a], line[2 * a + 1]], axis=0).astype(BF16)
            for a in range(len(line) // 2 - 1):
                odd_ref[q, h, pl.ds(16 * a, 16), :] = jnp.concatenate([line[2 * a + 1], line[2 * a + 2]], axis=0).astype(BF16)

    def multiply(q):
        acc = None
        for s in range(LAGS + 1):
            start = LAGS - s
            if start % 2 == 0:
                lhs = [even_ref[q, h, pl.ds(start * 8, rows), :] for h in range(2)]
            else:
                lhs = [odd_ref[q, h, pl.ds((start - 1) * 8, rows), :] for h in range(2)]
            lhs = jnp.concatenate(lhs, axis=1)
            t = 2 * s
            rhs = jnp.concatenate(
                [
                    jnp.concatenate([wide_ref[q, t + 1], wide_ref[q, t + 2]], axis=1),
                    jnp.concatenate([wide_ref[q, t], wide_ref[q, t + 1]], axis=1),
                ],
                axis=0,
            )
            term = jnp.dot(lhs, rhs, preferred_element_type=F32)
            acc = term if acc is None else acc + term
        mine = lax.broadcasted_iota(jnp.int32, (2, 128), 0) * 128 + lax.broadcasted_iota(jnp.int32, (2, 128), 1)
        mine = jnp.where(mine == q * sources + lax.axis_index("seq"), skip_ref[...], 0.0)
        skip = jnp.sum(jnp.sum(mine, axis=1, keepdims=True), axis=0, keepdims=True)
        for p in range(positions):
            for h in range(2):
                start = (p // 4) * chunk + q * 8 + (p % 4) * 2 + h
                own = flat_ref[pl.ds(start, 8, stride=pitch), :]
                out_rows[q, pl.ds((p * 2 + h) * 8, 8), :] = acc[8 * p:8 * p + 8, h * 128:(h + 1) * 128] + skip * own
    tokens, channels = og_ref.shape
    count = tokens // 128
    og_pitch = og_rows_ref.shape[0] // count
    eye = identity(channels)
    for b in range(0, count, 2):
        turned = flipped(eye, og_ref[pl.ds(b * 128, 256), :])
        for n in range(2):
            og_rows_ref[pl.ds((b + n) * og_pitch, channels), :] = turned[:, n * 128:(n + 1) * 128]

    def og_rows(first, last):
        for j in range(first, last):
            got = [og_rows_ref[pl.ds(q * sources + j, count, stride=og_pitch), :] for q in range(per_peer)]
            og_out_ref[pl.ds(j * 32, 32), :] = jnp.concatenate(got, axis=0).astype(BF16)

    toeplitz(0)
    signal(0)
    for q in range(per_peer):
        og_rows(q * sources // per_peer, (q + 1) * sources // per_peer)
        if q + 1 < per_peer:
            toeplitz(q + 1)
            signal(q + 1)
        multiply(q)

    for j in range(sources):
        g, jj = divmod(j, per_seg)
        got = [out_rows[q, pl.ds(jj * 64 + g, 8, stride=8), :] for q in range(per_peer)]
        out_ref[pl.ds(j * 32, 32), :] = jnp.concatenate(got, axis=0).astype(BF16)


def square_kernel(conv_ref, og_ref, square_ref):
    def step(n, total):
        part = pl.ds(pl.multiple_of(n * 128, 128), 128)
        mixed = conv_ref[part, :].astype(F32) * og_ref[part, :].astype(F32)
        return total + (mixed * mixed).reshape(8, 16, 128)

    total = lax.fori_loop(0, conv_ref.shape[0] // 128, step, jnp.zeros((8, 16, 128), F32), unroll=True)
    total = jnp.sum(total, axis=0)
    square_ref[...] = total[:8] + total[8:]


def mix_kernel(conv_ref, og_ref, mixed_ref, rows_ref):
    peers = conv_ref.shape[0] // 32
    count, channels, _ = mixed_ref.shape
    per_peer = channels // peers
    for j in range(peers):
        part = pl.ds(j * 32, 32)
        rows_ref[pl.ds(j * 40, 32), :] = conv_ref[part, :].astype(F32) * og_ref[part, :].astype(F32)
    for b in range(count):
        for q in range(per_peer):
            mixed_ref[b, pl.ds(q * peers, peers), :] = rows_ref[pl.ds(q * count + b, peers, stride=40), :]


def norm_kernel(mixed_ref, own_ref, first_ref, second_ref, third_ref, out_hbm, out_ref, sems):
    count = mixed_ref.shape[0]
    power = (own_ref[...] + first_ref[...] + second_ref[...] + third_ref[...]) * (1.0 / CH)
    scale = 1.0 / jnp.sqrt(power + 1e-05)
    eye = identity(128)
    copies = []
    for b in range(count):
        part = pl.ds(b * 128, 128)
        scaled = (mixed_ref[b] * scale[b:b + 1, :]).astype(BF16)
        out_ref[part, :] = flipped(eye, scaled).astype(BF16)
        copies.append(pltpu.make_async_copy(out_ref.at[part], out_hbm.at[part], sems.at[b]))
        copies[-1].start()
    for copy in copies:
        copy.wait()


def shape(dims, dtype):
    return jax.ShapeDtypeStruct(dims, dtype)


VMEM = pl.BlockSpec(memory_space=pltpu.VMEM)
SMEM = pl.BlockSpec(memory_space=pltpu.SMEM)
HBM = pl.BlockSpec(memory_space=pltpu.HBM)


def params(mib):
    return pltpu.CompilerParams(vmem_limit_bytes=mib * MIB)


def local(gate_in, value_in, out_gate, filter_taps, skip_gain):
    tokens, channels = gate_in.shape
    peers = lax.axis_size("seq")
    per_peer = channels // peers
    count = tokens // 128
    rows = peers * per_peer * count
    inputs = (gate_in, value_in, filter_taps, skip_gain.reshape(channels // 128, 128), out_gate)
    message, skip, og_here = pl.pallas_call(
        gate_kernel,
        out_shape=(shape((peers * 34, 128), BF16), shape((channels // 128, 128), F32), shape((tokens, channels), BF16)),
        in_specs=[HBM] * 5,
        out_specs=(VMEM,) * 3,
        scratch_shapes=[
            pltpu.VMEM((tokens, channels), BF16),
            pltpu.VMEM((tokens, channels), BF16),
            pltpu.VMEM(filter_taps.shape, BF16),
            pltpu.VMEM(((2 * count + 8) * (channels + 8) + 16 * (peers + 8), 128), F32),
            pltpu.SemaphoreType.DMA((3, tokens // 256)),
        ],
        compiler_params=params(16),
        name="gate",
    )(*(pltpu.with_memory_space_constraint(a, pltpu.HBM) for a in inputs))
    message = lax.all_to_all(message.reshape(peers, 17, 2, 128), "seq", split_axis=0, concat_axis=0, tiled=True)
    convolved, turned = pl.pallas_call(
        conv_kernel,
        out_shape=(shape((rows, 128), BF16), shape((rows, 128), BF16)),
        in_specs=[VMEM] * 3,
        out_specs=(VMEM, VMEM),
        scratch_shapes=[
            pltpu.VMEM((count * (channels + 8), 128), F32),
            pltpu.VMEM((SEGS * 276, 128), F32),
            pltpu.VMEM((4, 32, 128), F32),
            pltpu.VMEM((4, 2, 384, 128), BF16),
            pltpu.VMEM((4, 2, 384, 128), BF16),
            pltpu.VMEM((4, 34, 16, 128), BF16),
            pltpu.VMEM((4, 256, 256), BF16),
            pltpu.VMEM((4, 35, 128, 128), BF16),
            pltpu.VMEM((4, 512, 128), F32),
        ],
        compiler_params=params(24),
        name="conv",
    )(skip, message.reshape(peers * 34, 128), og_here)
    convolved = lax.all_to_all(
        convolved.reshape(peers, 32, 128), "seq", split_axis=0, concat_axis=0, tiled=True
    ).reshape(rows, 128)
    squares = pl.pallas_call(
        square_kernel,
        out_shape=shape((count, 128), F32),
        in_specs=[VMEM] * 2,
        out_specs=VMEM,
        compiler_params=params(8),
        name="square",
    )(convolved, turned)
    group = lax.axis_size("mp")
    others = [lax.ppermute(squares, "mp", [(i, (i + k) % group) for i in range(group)]) for k in range(1, group)]
    mixed = pl.pallas_call(
        mix_kernel,
        out_shape=shape((count, channels, 128), F32),
        in_specs=[VMEM] * 2,
        out_specs=VMEM,
        scratch_shapes=[pltpu.VMEM((peers * 40, 128), F32)],
        compiler_params=params(8),
        cost_estimate=pl.CostEstimate(flops=20000000, bytes_accessed=8 * tokens * channels, transcendentals=0),
        name="mix",
    )(convolved, turned)
    return pl.pallas_call(
        norm_kernel,
        out_shape=shape((tokens, channels), BF16),
        in_specs=[VMEM] * 5,
        out_specs=HBM,
        scratch_shapes=[pltpu.VMEM((tokens, channels), BF16), pltpu.SemaphoreType.DMA((count,))],
        compiler_params=params(8),
        name="norm",
    )(mixed, squares, *others)


def solution(mesh):
    return jax.shard_map(
        local,
        mesh=mesh,
        in_specs=(P("seq", "mp"), P("seq", "mp"), P("seq", "mp"), P("seq", "mp"), P("mp")),
        out_specs=P("seq", "mp"),
        check_vma=False,
    )
```
